8 devices in a mesh: dp: 1 (over z), my: 2 (over y), mx: 4 (over x, core).
Axes of the slice: x: 2, y: 2, z: 1, core: 2. Of those that a mesh axis runs over, the one named last changes fastest.
Arguments:
- x_in: bfloat16 [4096, 2048], P('dp', 'my')
- gain_attn: bfloat16 [2048], P('my')
- w_q: bfloat16 [2048, 32, 64], P('my', 'mx')
- w_k: bfloat16 [2048, 8, 64], P('my', 'mx')
- w_v: bfloat16 [2048, 8, 64], P('my', 'mx')
- w_o: bfloat16 [32, 64, 2048], P('mx', None, 'my')
- gain_mlp: bfloat16 [2048], P('my')
- w_gate: bfloat16 [2048, 8192], P('my', 'mx')
- w_up: bfloat16 [2048, 8192], P('my', 'mx')
- w_down: bfloat16 [8192, 2048], P('mx', 'my')
Outputs:
- output: bfloat16 [4096, 2048], P('dp', 'my')
All inputs are finite; a program needn't handle non-finite values.
Results may differ from the reference program's by a relative error of at most 0.0123224.
Values are sent between devices in bfloat16 or wider.
A program may use at most 1 GiB of HBM per device.

```python
import jax
import jax.numpy as jnp
from jax import lax

TOKENS = 4096
D = 2048
HEADS = 32
KV_HEADS = 8
HEAD = 64
FF = 8192

ROPE_BASE = 10000.0
NORM_EPS = 1e-6
QBLOCK = min(TOKENS, 128)
GROUPS = HEADS // KV_HEADS
HALF_DIM = HEAD // 2


def weight_normal(key_w, fan_in, shape_w):
    return (jax.random.normal(key_w, shape_w, jnp.float32) * fan_in ** -0.5).astype(jnp.bfloat16)


def setup_inputs(seed: int = 0, part: int = 0) -> dict:
    base_key = jax.random.key(seed)
    part_keys = jax.random.split(jax.random.fold_in(base_key, part), 4)
    shared_keys = jax.random.split(base_key, 9)
    col_frac = jnp.arange(D, dtype=jnp.float32) / D
    slope_val = jax.random.uniform(part_keys[0], (), jnp.float32, 1.5, 2.5)
    col_scale = jnp.exp(slope_val * (col_frac - 0.5) - 0.2)
    phase_start = jax.random.uniform(part_keys[1], (), jnp.float32, 0.0, 6.28)
    phase_t = 3.0 * jnp.arange(TOKENS, dtype=jnp.float32) / TOKENS + phase_start
    drift_dirs = jax.random.normal(part_keys[2], (2, D), jnp.float32)
    drift_val = jnp.cos(phase_t)[:, None] * drift_dirs[0][None, :] + jnp.sin(phase_t)[:, None] * drift_dirs[1][None, :]
    noise_val = jax.random.normal(part_keys[3], (TOKENS, D), jnp.float32)
    x_in = (col_scale[None, :] * (noise_val + 0.8 * drift_val)).astype(jnp.bfloat16)
    gain_attn = (0.5 + jax.random.uniform(shared_keys[0], (D,), jnp.float32)).astype(jnp.bfloat16)
    w_q = weight_normal(shared_keys[1], D, (D, HEADS, HEAD))
    w_k = weight_normal(shared_keys[2], D, (D, KV_HEADS, HEAD))
    w_v = weight_normal(shared_keys[3], D, (D, KV_HEADS, HEAD))
    w_o = weight_normal(shared_keys[4], HEADS * HEAD, (HEADS, HEAD, D))
    gain_mlp = (0.5 + jax.random.uniform(shared_keys[5], (D,), jnp.float32)).astype(jnp.bfloat16)
    w_gate = weight_normal(shared_keys[6], D, (D, FF))
    w_up = weight_normal(shared_keys[7], D, (D, FF))
    w_down = weight_normal(shared_keys[8], FF, (FF, D))
    return {"x_in": x_in, "gain_attn": gain_attn, "w_q": w_q, "w_k": w_k, "w_v": w_v, "w_o": w_o, "gain_mlp": gain_mlp, "w_gate": w_gate, "w_up": w_up, "w_down": w_down}


def rms_norm(values, gain):
    values_f = values.astype(jnp.float32)
    mean_sq = jnp.mean(values_f * values_f, axis=-1, keepdims=True)
    return (values_f * lax.rsqrt(mean_sq + NORM_EPS) * gain.astype(jnp.float32)).astype(jnp.bfloat16)


def apply_rope(values, positions):
    inv_freq = ROPE_BASE ** (-jnp.arange(HALF_DIM, dtype=jnp.float32) / HALF_DIM)
    angles = positions[:, None] * inv_freq[None, :]
    cos_t = jnp.cos(angles)[:, None, :]
    sin_t = jnp.sin(angles)[:, None, :]
    values_f = values.astype(jnp.float32)
    first_half = values_f[..., :HALF_DIM]
    second_half = values_f[..., HALF_DIM:]
    return jnp.concatenate([first_half * cos_t - second_half * sin_t, second_half * cos_t + first_half * sin_t], axis=-1).astype(jnp.bfloat16)


def reference(x_in, gain_attn, w_q, w_k, w_v, w_o, gain_mlp, w_gate, w_up, w_down):
    normed = rms_norm(x_in, gain_attn)
    q_heads = jnp.dot(normed, w_q.reshape(D, HEADS * HEAD), preferred_element_type=jnp.float32).astype(jnp.bfloat16).reshape(TOKENS, HEADS, HEAD)
    k_heads = jnp.dot(normed, w_k.reshape(D, KV_HEADS * HEAD), preferred_element_type=jnp.float32).astype(jnp.bfloat16).reshape(TOKENS, KV_HEADS, HEAD)
    v_heads = jnp.dot(normed, w_v.reshape(D, KV_HEADS * HEAD), preferred_element_type=jnp.float32).astype(jnp.bfloat16).reshape(TOKENS, KV_HEADS, HEAD)
    positions = jnp.arange(TOKENS, dtype=jnp.float32)
    q_rot = apply_rope(q_heads, positions)
    k_float = apply_rope(k_heads, positions).astype(jnp.float32)
    v_float = v_heads.astype(jnp.float32)
    q_blocks = q_rot.reshape(TOKENS // QBLOCK, QBLOCK, KV_HEADS, GROUPS, HEAD)
    key_pos = jnp.arange(TOKENS)

    def attend(blk_args):
        q_blk, blk_idx = blk_args
        scores = jnp.einsum("qkgd,tkd->qkgt", q_blk.astype(jnp.float32), k_float) * HEAD ** -0.5
        query_pos = blk_idx * QBLOCK + jnp.arange(QBLOCK)
        causal = key_pos[None, :] <= query_pos[:, None]
        scores = jnp.where(causal[:, None, None, :], scores, -jnp.inf)
        attn_prob = jax.nn.softmax(scores, axis=-1).astype(jnp.bfloat16)
        blk_out = jnp.einsum("qkgt,tkd->qkgd", attn_prob.astype(jnp.float32), v_float)
        return blk_out.astype(jnp.bfloat16).reshape(QBLOCK, HEADS * HEAD)

    attn_heads = lax.map(attend, (q_blocks, jnp.arange(TOKENS // QBLOCK))).reshape(TOKENS, HEADS * HEAD)
    attn_proj = jnp.dot(attn_heads, w_o.reshape(HEADS * HEAD, D), preferred_element_type=jnp.float32)
    residual = (x_in.astype(jnp.float32) + attn_proj).astype(jnp.bfloat16)
    normed_mlp = rms_norm(residual, gain_mlp)
    gate_val = jnp.dot(normed_mlp, w_gate, preferred_element_type=jnp.float32)
    up_val = jnp.dot(normed_mlp, w_up, preferred_element_type=jnp.float32)
    act_val = (jax.nn.silu(gate_val) * up_val).astype(jnp.bfloat16)
    down_val = jnp.dot(act_val, w_down, preferred_element_type=jnp.float32)
    return (residual.astype(jnp.float32) + down_val).astype(jnp.bfloat16)
```

```python
import functools

import jax
import jax.numpy as jnp
from jax import lax
from jax.experimental import pallas as pl
from jax.experimental.pallas import tpu as pltpu
from jax.sharding import PartitionSpec as P

ROPE_BASE = 10000.0
NORM_EPS = 1e-6
F32 = jnp.float32
BF16 = jnp.bfloat16


CHUNKS = 4
BQ = 256
BK = 512
VROWS = 80


def dot(a, b):
    return jnp.dot(a, b, preferred_element_type=F32)


def whole(shape):
    return pl.BlockSpec(shape, lambda *_: (0,) * len(shape), pipeline_mode=pl.Buffered(1))


def qkv_kernel(xa_ref, xb_ref, wa_ref, wb_ref, gain_ref, cos_ref, sin_ref, q_ref, k_ref, vt_ref):
    width = 2 * xa_ref.shape[1]
    xa = xa_ref[...].astype(F32)
    xb = xb_ref[...].astype(F32)
    row_sq = jnp.sum(xa * xa, axis=-1, keepdims=True) + jnp.sum(xb * xb, axis=-1, keepdims=True)
    scale = lax.rsqrt(row_sq / width + NORM_EPS)
    na = (xa * scale * gain_ref[0:1, :].astype(F32)).astype(BF16)
    nb = (xb * scale * gain_ref[1:2, :].astype(F32)).astype(BF16)
    qkv = (dot(na, wa_ref[...]) + dot(nb, wb_ref[...])).astype(BF16)
    cos_t = cos_ref[...]
    sin_t = sin_ref[...]
    lane = lax.broadcasted_iota(jnp.int32, cos_t.shape, 1)
    first = (lane % 64) < 32

    def rotate(v):
        v = v.astype(F32)
        swapped = jnp.where(first, pltpu.roll(v, 96, 1), pltpu.roll(v, 32, 1))
        return (v * cos_t + swapped * sin_t).astype(BF16)

    for j in range(4):
        q_ref[:, j * 128 : (j + 1) * 128] = rotate(qkv[:, j * 128 : (j + 1) * 128]) * jnp.asarray(0.125, BF16)
    kr = rotate(qkv[:, 512:640])
    k_ref[0] = kr[:, :64]
    k_ref[1] = kr[:, 64:]
    vt = qkv[:, 640:768].astype(F32).T.astype(BF16)
    pad = (lax.broadcasted_iota(jnp.int32, (VROWS - 64, vt.shape[1]), 0) == 0).astype(F32).astype(BF16)
    for g in range(2):
        vt_ref[g, :64, :] = vt[g * 64 : (g + 1) * 64, :]
        vt_ref[g, 64:, :] = pad


def qkv_call(xa, xb, wa, wb, gains, cos_t, sin_t):
    tokens, half = xa.shape
    bt = 512
    return pl.pallas_call(
        qkv_kernel,
        grid=(tokens // bt,),
        in_specs=[
            pl.BlockSpec((bt, half), lambda i: (i, 0)),
            pl.BlockSpec((bt, half), lambda i: (i, 0)),
            whole((half, 768)),
            whole((half, 768)),
            whole((2, half)),
            pl.BlockSpec((bt, 128), lambda i: (i, 0)),
            pl.BlockSpec((bt, 128), lambda i: (i, 0)),
        ],
        out_specs=[
            pl.BlockSpec((bt, 512), lambda i: (i, 0)),
            pl.BlockSpec((2, bt, 64), lambda i: (0, i, 0)),
            pl.BlockSpec((2, VROWS, bt), lambda i: (0, 0, i)),
        ],
        out_shape=[
            jax.ShapeDtypeStruct((tokens, 512), BF16),
            jax.ShapeDtypeStruct((2, tokens, 64), BF16),
            jax.ShapeDtypeStruct((2, VROWS, tokens), BF16),
        ],
        cost_estimate=pl.CostEstimate(flops=2 * tokens * 2 * half * 768, bytes_accessed=tokens * 6000, transcendentals=0),
        name="qkv",
    )(xa, xb, wa, wb, gains, cos_t, sin_t)


def attn_kernel(base, nb, meta_ref, q_ref, k_ref, vt_ref, own_ref, mate_ref, acc_ref):
    i = pl.program_id(0)
    qb = q_block(base, nb, i, meta_ref)
    q_heads = [q_ref[:, h * 64 : (h + 1) * 64] for h in range(4)]
    acc_ref[...] = jnp.zeros_like(acc_ref)

    def step(j, ms, masked):
        start = pl.multiple_of(j * BK, BK)
        kj = k_ref[0, pl.ds(start, BK), :]
        vj = vt_ref[0, :, pl.ds(start, BK)]
        out = []
        for h in range(4):
            s = lax.dot_general(kj, q_heads[h], (((1,), (1,)), ((), ())), preferred_element_type=F32)
            if masked:
                key_pos = start + lax.broadcasted_iota(jnp.int32, s.shape, 0)
                query_pos = qb * BQ + lax.broadcasted_iota(jnp.int32, s.shape, 1)
                s = jnp.where(key_pos <= query_pos, s, -jnp.inf)
            m_new = jnp.maximum(ms[h], jnp.max(s, axis=0, keepdims=True))
            p = jnp.exp(s - m_new).astype(BF16)
            acc_ref[h] = acc_ref[h] * jnp.exp(ms[h] - m_new) + dot(vj, p)
            out.append(m_new)
        return tuple(out)

    ms = tuple(jnp.full((1, BQ), -jnp.inf, F32) for _ in range(4))
    n_full = (qb * BQ) // BK
    ms = lax.fori_loop(0, n_full, lambda j, c: step(j, c, False), ms)
    step(n_full, ms, True)
    heads = [acc_ref[h, :64, :] / acc_ref[h, 64:65, :] for h in range(4)]
    o = jnp.concatenate(heads, axis=0).T.astype(BF16)

    @pl.when(i < nb // 2)
    def _():
        own_ref[...] = o

    @pl.when(i >= nb // 2)
    def _():
        mate_ref[...] = o


def q_block(base, nb, i, meta_ref):
    core = meta_ref[0]
    rel = i // (nb // 2)
    half = core + rel - 2 * core * rel
    return base + half * (nb // 2) + i % (nb // 2)


def attn_call(chunk, t_chunk, core, q, k, vt):
    tokens = q.shape[0]
    nb = t_chunk // BQ
    base = chunk * nb
    hb = nb // 2
    half = t_chunk // 2
    pairs = 8 * t_chunk * (chunk * t_chunk + t_chunk // 2)
    return pl.pallas_call(
        functools.partial(attn_kernel, base, nb),
        grid_spec=pltpu.PrefetchScalarGridSpec(
            num_scalar_prefetch=1,
            grid=(nb, 2),
            in_specs=[
                pl.BlockSpec((BQ, 256), lambda i, g, meta: (q_block(base, nb, i, meta), g)),
                pl.BlockSpec((1, tokens, 64), lambda i, g, meta: (g, 0, 0)),
                pl.BlockSpec((1, VROWS, tokens), lambda i, g, meta: (g, 0, 0)),
            ],
            out_specs=[
                pl.BlockSpec((BQ, 256), lambda i, g, meta: (jnp.minimum(i, hb - 1), jnp.where(i < hb, g, 1))),
                pl.BlockSpec((BQ, 256), lambda i, g, meta: (jnp.maximum(i - hb, 0), jnp.where(i < hb, 0, g))),
            ],
            scratch_shapes=[pltpu.VMEM((4, VROWS, BQ), F32)],
        ),
        out_shape=[jax.ShapeDtypeStruct((half, 512), BF16)] * 2,
        cost_estimate=pl.CostEstimate(flops=pairs * 700, bytes_accessed=t_chunk * 4096, transcendentals=pairs),
        name="attn",
    )(core, q, k, vt)


def oproj_kernel(meta_ref, o0_ref, o1_ref, o2_ref, o3_ref, xa_ref, xb_ref, wa_ref, wb_ref, gain_ref, h_ref, m_ref, o_all):
    me = meta_ref[1]
    half = xa_ref.shape[1]
    for j, ref in enumerate((o0_ref, o1_ref, o2_ref, o3_ref)):
        slot = meta_ref[2 + j]
        o_all[:, pl.ds(pl.multiple_of(slot * 512, 512), 512)] = ref[...]
    o = o_all[...]
    ha = (xa_ref[...].astype(F32) + dot(o, wa_ref[...])).astype(BF16)
    hb = (xb_ref[...].astype(F32) + dot(o, wb_ref[...])).astype(BF16)
    h_ref[...] = ha
    ha = ha.astype(F32)
    hb = hb.astype(F32)
    row_sq = jnp.sum(ha * ha, axis=-1, keepdims=True) + jnp.sum(hb * hb, axis=-1, keepdims=True)
    scale = lax.rsqrt(row_sq / (2 * half) + NORM_EPS)
    m_ref[:, :half] = (ha * scale * gain_ref[0:1, :].astype(F32)).astype(BF16)
    m_ref[:, half:] = (hb * scale * gain_ref[1:2, :].astype(F32)).astype(BF16)


def oproj_call(chunk, t_chunk, meta, o_parts, xa, xb, wa, wb, gains):
    half = xa.shape[1]
    t_half = t_chunk // 2
    bt = min(256, t_half)
    nb = t_half // bt
    o_spec = pl.BlockSpec((bt, 512), lambda i, meta: (i, 0))
    x_spec = pl.BlockSpec((bt, half), lambda i, meta: (chunk * 2 * nb + meta[0] * nb + i, 0))
    return pl.pallas_call(
        oproj_kernel,
        grid_spec=pltpu.PrefetchScalarGridSpec(
            num_scalar_prefetch=1,
            grid=(nb,),
            in_specs=[o_spec] * 4 + [x_spec] * 2 + [whole((2 * half, half))] * 2 + [whole((2, half))],
            out_specs=[
                pl.BlockSpec((bt, half), lambda i, meta: (i, 0)),
                pl.BlockSpec((bt, 2 * half), lambda i, meta: (i, 0)),
            ],
            scratch_shapes=[pltpu.VMEM((bt, 2048), BF16)],
        ),
        out_shape=[jax.ShapeDtypeStruct((t_half, half), BF16), jax.ShapeDtypeStruct((t_half, 2 * half), BF16)],
        cost_estimate=pl.CostEstimate(flops=2 * t_half * 2048 * 2048, bytes_accessed=t_half * 8192, transcendentals=0),
        name="oproj",
    )(meta, *o_parts, xa, xb, wa, wb, gains)


def mlp_kernel(nb, mo_ref, mm_ref, ga_ref, gb_ref, ua_ref, ub_ref, da_ref, db_ref, own_ref, mate_ref):
    i = pl.program_id(0)
    half = ga_ref.shape[0]
    m = jnp.where(i < nb, mo_ref[...], mm_ref[...])
    ma = m[:, :half]
    mb = m[:, half:]
    gate = dot(ma, ga_ref[...]) + dot(mb, gb_ref[...])
    up = dot(ma, ua_ref[...]) + dot(mb, ub_ref[...])
    act = (jax.nn.silu(gate) * up).astype(BF16)
    pa = dot(act, da_ref[...]).astype(BF16)
    pb = dot(act, db_ref[...]).astype(BF16)

    @pl.when(i < nb)
    def _():
        own_ref[:, :half] = pa
        own_ref[:, half:] = pb

    @pl.when(i >= nb)
    def _():
        mate_ref[:, :half] = pa
        mate_ref[:, half:] = pb


def mlp_call(m_own, m_mate, ga, gb, ua, ub, da, db):
    t_half, width = m_own.shape
    half = width // 2
    hid = ga.shape[1]
    bt = min(256, t_half)
    nb = t_half // bt
    own_spec = pl.BlockSpec((bt, width), lambda i: (jnp.minimum(i, nb - 1), 0))
    mate_spec = pl.BlockSpec((bt, width), lambda i: (jnp.maximum(i - nb, 0), 0))
    return pl.pallas_call(
        functools.partial(mlp_kernel, nb),
        grid=(2 * nb,),
        in_specs=[own_spec, mate_spec] + [whole((half, hid))] * 4 + [whole((hid, half))] * 2,
        out_specs=[own_spec, mate_spec],
        out_shape=[jax.ShapeDtypeStruct((t_half, width), BF16)] * 2,
        cost_estimate=pl.CostEstimate(flops=2 * 2 * t_half * width * hid * 3, bytes_accessed=t_half * 16384, transcendentals=2 * t_half * hid),
        name="mlp",
    )(m_own, m_mate, ga, gb, ua, ub, da, db)


def solution(mesh):
    mx_size = mesh.shape["mx"]
    swap_y = [(0, 1), (1, 0)]
    swap_x = [(d, d ^ 2) for d in range(mx_size)]
    swap_c = [(d, d ^ 1) for d in range(mx_size)]
    swap_xc = [(d, d ^ 3) for d in range(mx_size)]

    def send(name, v, axis, perm):
        with jax.named_scope(name):
            return lax.ppermute(v, axis, perm)

    def local_layer(x_in, gain_attn, w_q, w_k, w_v, w_o, gain_mlp, w_gate, w_up, w_down):
        tokens, half = x_in.shape
        row = lax.axis_index("my")
        me = lax.axis_index("mx")
        core = lax.rem(me, 2)
        meta = jnp.stack([core, me, me, me ^ 1, me ^ 2, me ^ 3]).astype(jnp.int32)
        core_arr = jnp.reshape(core, (1,)).astype(jnp.int32)

        quarter = tokens // mx_size
        sub = quarter // 2
        x_oth = jnp.zeros_like(x_in)
        for s in range(2):
            mine = lax.dynamic_slice(x_in, (me * quarter + s * sub, 0), (sub, half))
            got_y = send(f"xy{s}", mine, "my", swap_y)
            got_x = send(f"xx{s}", got_y, "mx", swap_x)
            got_c = send(f"xc{s}", got_y, "mx", swap_c)
            got_xc = send(f"xd{s}", got_x, "mx", swap_c)
            for d, piece in ((0, got_y), (1, got_c), (2, got_x), (3, got_xc)):
                x_oth = lax.dynamic_update_slice(x_oth, piece, ((me ^ d) * quarter + s * sub, 0))

        gains = jnp.stack([gain_attn, gain_mlp])
        gains_oth = send("gains", gains, "my", swap_y)
        gains_a = jnp.stack([gain_attn, gains_oth[0]])
        gains_m = jnp.stack([gain_mlp, gains_oth[1]])
        w_qkv = jnp.concatenate([w_q.reshape(half, 512), w_k.reshape(half, 128), w_v.reshape(half, 128)], axis=1)
        w_qkv_oth = send("wqkv", w_qkv, "my", swap_y)

        wo_own = w_o.reshape(512, half)
        wo_oth = send("woy", wo_own, "my", swap_y)
        parts = jnp.stack([wo_own, wo_oth])
        parts_x = jnp.stack([send("woxa", wo_own, "mx", swap_x), send("woxb", wo_oth, "mx", swap_x)])
        parts_c = send("woc", parts, "mx", swap_c)
        parts_xc = send("wod", parts_x, "mx", swap_c)
        wo_all = jnp.zeros((2, 2048, half), BF16)
        for d, piece in ((0, parts), (1, parts_c), (2, parts_x), (3, parts_xc)):
            wo_all = lax.dynamic_update_slice(wo_all, piece, (0, (me ^ d) * 512, 0))
        wo_a, wo_b = wo_all[0], wo_all[1]

        hid = w_gate.shape[1] // 2
        keep, give = row * hid, (1 - row) * hid
        ga = lax.dynamic_slice(w_gate, (0, keep), (half, hid))
        ua = lax.dynamic_slice(w_up, (0, keep), (half, hid))
        da = lax.dynamic_slice(w_down, (keep, 0), (hid, half))
        gb = send("wgate", lax.dynamic_slice(w_gate, (0, give), (half, hid)), "my", swap_y)
        ub = send("wup", lax.dynamic_slice(w_up, (0, give), (half, hid)), "my", swap_y)
        db = send("wdown", lax.dynamic_slice(w_down, (give, 0), (hid, half)), "my", swap_y)

        half_dim = 32
        inv_freq = ROPE_BASE ** (-jnp.arange(half_dim, dtype=F32) / half_dim)
        angles = jnp.arange(tokens, dtype=F32)[:, None] * inv_freq[None, :]
        cos_t = jnp.cos(angles)
        sin_t = jnp.sin(angles)
        cos_t = jnp.concatenate([cos_t] * 4, axis=1)
        sin_t = jnp.concatenate([-sin_t, sin_t] * 2, axis=1)

        q, k, vt = qkv_call(x_in, x_oth, w_qkv, w_qkv_oth, gains_a, cos_t, sin_t)

        t_chunk = tokens // CHUNKS
        t_half = t_chunk // 2
        y_out = jnp.zeros_like(x_in)
        for ch in range(CHUNKS):
            o_own, o_mate = attn_call(ch, t_chunk, core_arr, q, k, vt)
            o_c = send(f"oc{ch}", o_mate, "mx", swap_c)
            o_x = send(f"ox{ch}", o_own, "mx", swap_x)
            o_xc = send(f"od{ch}", o_mate, "mx", swap_xc)
            h_own, m_own = oproj_call(ch, t_chunk, meta, (o_own, o_c, o_x, o_xc), x_in, x_oth, wo_a, wo_b, gains_m)
            m_mate = send(f"mc{ch}", m_own, "mx", swap_c)
            p_own, p_mate = mlp_call(m_own, m_mate, ga, gb, ua, ub, da, db)
            p_recv = send(f"pc{ch}", p_mate, "mx", swap_c)
            s_a = (p_own[:, :half].astype(F32) + p_recv[:, :half].astype(F32)).astype(BF16)
            s_b = (p_own[:, half:].astype(F32) + p_recv[:, half:].astype(F32)).astype(BF16)
            r_y = send(f"py{ch}", s_b, "my", swap_y)
            z_own = (s_a.astype(F32) + r_y.astype(F32)).astype(BF16)
            z_x = send(f"px{ch}", z_own, "mx", swap_x)
            y_own = (h_own.astype(F32) + (z_own.astype(F32) + z_x.astype(F32))).astype(BF16)
            y_mate = send(f"yc{ch}", y_own, "mx", swap_c)
            y_out = lax.dynamic_update_slice(y_out, y_own, (ch * t_chunk + core * t_half, 0))
            y_out = lax.dynamic_update_slice(y_out, y_mate, (ch * t_chunk + (1 - core) * t_half, 0))
        return y_out

    in_specs = (P("dp", "my"), P("my"), P("my", "mx", None), P("my", "mx", None), P("my", "mx", None), P("mx", None, "my"), P("my"), P("my", "mx"), P("my", "mx"), P("mx", "my"))
    return jax.shard_map(local_layer, mesh=mesh, in_specs=in_specs, out_specs=P("dp", "my"), check_vma=False)
```

```python
import functools

import jax
import jax.numpy as jnp
from jax import lax
from jax.experimental import pallas as pl
from jax.experimental.pallas import tpu as pltpu
from jax.sharding import PartitionSpec as P


ROPE_BASE = 10000.0
NORM_EPS = 1e-6
F32 = jnp.float32
BF16 = jnp.bfloat16


CHUNKS = 4
OUT_SUBS = 2
BQ = 256
BK = 512
VROWS = 80


def dot(a, b):
    return jnp.dot(a, b, preferred_element_type=F32)


def whole(shape):
    return pl.BlockSpec(shape, lambda *_: (0,) * len(shape), pipeline_mode=pl.Buffered(1))


HBM = pl.BlockSpec(memory_space=pl.ANY)


def qkv_kernel(meta_ref, xa_ref, p0_ref, p1_ref, p2_ref, p3_ref, wa_ref, wb_ref, gain_ref, cos_ref, sin_ref, *rest):
    q_ref, k_ref, vt_ref, xo_ref = rest[-4:]
    i = pl.program_id(0)
    for d, ref in enumerate((p0_ref, p1_ref, p2_ref, p3_ref)):

        @pl.when(i == d)
        def _():
            xo_ref[...] = ref[...]

    width = 2 * xa_ref.shape[1]
    xa = xa_ref[...].astype(F32)
    xb = xo_ref[...].astype(F32)
    row_sq = jnp.sum(xa * xa, axis=-1, keepdims=True) + jnp.sum(xb * xb, axis=-1, keepdims=True)
    scale = lax.rsqrt(row_sq / width + NORM_EPS)
    na = (xa * scale * gain_ref[0:1, :].astype(F32)).astype(BF16)
    nb = (xb * scale * gain_ref[1:2, :].astype(F32)).astype(BF16)
    qkv = (dot(na, wa_ref[...]) + dot(nb, wb_ref[...])).astype(BF16)
    cos_t = cos_ref[...]
    sin_t = sin_ref[...]
    lane = lax.broadcasted_iota(jnp.int32, cos_t.shape, 1)
    first = (lane % 64) < 32

    def rotate(v):
        v = v.astype(F32)
        swapped = jnp.where(first, pltpu.roll(v, 96, 1), pltpu.roll(v, 32, 1))
        return (v * cos_t + swapped * sin_t).astype(BF16)

    for j in range(4):
        q_ref[:, j * 128 : (j + 1) * 128] = rotate(qkv[:, j * 128 : (j + 1) * 128]) * jnp.asarray(0.125, BF16)
    kr = rotate(qkv[:, 512:640])
    k_ref[0] = kr[:, :64]
    k_ref[1] = kr[:, 64:]
    vt = qkv[:, 640:768].astype(F32).T.astype(BF16)
    pad = (lax.broadcasted_iota(jnp.int32, (VROWS - 64, vt.shape[1]), 0) == 0).astype(F32).astype(BF16)
    for g in range(2):
        vt_ref[g, :64, :] = vt[g * 64 : (g + 1) * 64, :]
        vt_ref[g, 64:, :] = pad


def qkv_call(chunk, meta, xa, pieces, wa, wb, gains, cos_t, sin_t, prev):
    tokens, half = xa.shape
    bt = pieces[0].shape[0]

    def blk(i, meta):
        return chunk * 4 + meta[2 + i]

    row = lambda i, meta: (blk(i, meta), 0)
    outs = [
        jax.ShapeDtypeStruct((tokens, 512), BF16),
        jax.ShapeDtypeStruct((2, tokens, 64), BF16),
        jax.ShapeDtypeStruct((2, VROWS, tokens), BF16),
        jax.ShapeDtypeStruct((tokens, half), BF16),
    ]
    args = [xa, *pieces, wa, wb, gains, cos_t, sin_t]
    aliases = {}
    if prev is not None:
        aliases = {1 + len(args) + j: j for j in range(4)}
        args += list(prev)
    return pl.pallas_call(
        qkv_kernel,
        grid_spec=pltpu.PrefetchScalarGridSpec(
            num_scalar_prefetch=1,
            grid=(4,),
            in_specs=[pl.BlockSpec((bt, half), row)]
            + [whole((bt, half))] * 4
            + [whole((half, 768)), whole((half, 768)), whole((2, half))]
            + [pl.BlockSpec((bt, 128), row)] * 2
            + ([HBM] * 4 if prev is not None else []),
            out_specs=[
                pl.BlockSpec((bt, 512), row),
                pl.BlockSpec((2, bt, 64), lambda i, meta: (0, blk(i, meta), 0)),
                pl.BlockSpec((2, VROWS, bt), lambda i, meta: (0, 0, blk(i, meta))),
                pl.BlockSpec((bt, half), row),
            ],
        ),
        out_shape=outs,
        input_output_aliases=aliases,
        cost_estimate=pl.CostEstimate(flops=2 * 4 * bt * 2 * half * 768, bytes_accessed=4 * bt * 9000, transcendentals=0),
        name="qkv",
    )(meta, *args)


def attn_kernel(base, nb, meta_ref, q_ref, k_ref, vt_ref, own_ref, mate_ref, s_ref, acc_ref):
    i = pl.program_id(0)
    qb = q_block(base, nb, i, meta_ref)
    q_heads = [q_ref[:, h * 64 : (h + 1) * 64] for h in range(4)]
    acc_ref[...] = jnp.zeros_like(acc_ref)

    def scores(h, j, masked):
        start = pl.multiple_of(j * BK, BK)
        kj = k_ref[0, pl.ds(start, BK), :]
        s = lax.dot_general(kj, q_heads[h], (((1,), (1,)), ((), ())), preferred_element_type=F32)
        if masked:
            key_pos = start + lax.broadcasted_iota(jnp.int32, s.shape, 0)
            query_pos = qb * BQ + lax.broadcasted_iota(jnp.int32, s.shape, 1)
            s = jnp.where(key_pos <= query_pos, s, -jnp.inf)
        s_ref[h] = s
        return jnp.max(s, axis=0, keepdims=True)

    def weigh(h, j, m_old, m_blk):
        vj = vt_ref[0, :, pl.ds(pl.multiple_of(j * BK, BK), BK)]
        m_new = jnp.maximum(m_old, m_blk)
        p = jnp.exp(s_ref[h] - m_new).astype(BF16)
        acc_ref[h] = acc_ref[h] * jnp.exp(m_old - m_new) + dot(vj, p)
        return m_new

    n_full = (qb * BQ) // BK
    m_run = tuple(jnp.full((1, BQ), -jnp.inf, F32) for _ in range(4))
    m_blk = tuple(scores(h, n_full, True) for h in range(4))

    def body(j, carry):
        m_run, m_blk = carry
        prev = jnp.where(j == 0, n_full, j - 1)
        new_run, new_blk = [], []
        for h in range(4):
            new_run.append(weigh(h, prev, m_run[h], m_blk[h]))
            new_blk.append(scores(h, j, False))
        return tuple(new_run), tuple(new_blk)

    m_run, m_blk = lax.fori_loop(0, n_full, body, (m_run, m_blk))
    last = jnp.where(n_full == 0, n_full, n_full - 1)
    for h in range(4):
        weigh(h, last, m_run[h], m_blk[h])
    heads = [acc_ref[h, :64, :] / acc_ref[h, 64:65, :] for h in range(4)]
    o = jnp.concatenate(heads, axis=0).T.astype(BF16)

    @pl.when(i < nb // 2)
    def _():
        own_ref[...] = o

    @pl.when(i >= nb // 2)
    def _():
        mate_ref[...] = o


def q_block(base, nb, i, meta_ref):
    core = meta_ref[0]
    rel = i // (nb // 2)
    half = core + rel - 2 * core * rel
    return base + half * (nb // 2) + i % (nb // 2)


def attn_call(chunk, t_chunk, meta, q, k, vt):
    nb = t_chunk // BQ
    base = chunk * nb
    hb = nb // 2
    half = t_chunk // 2
    keys = (chunk + 1) * t_chunk
    pairs = 8 * t_chunk * (chunk * t_chunk + t_chunk // 2)
    return pl.pallas_call(
        functools.partial(attn_kernel, base, nb),
        grid_spec=pltpu.PrefetchScalarGridSpec(
            num_scalar_prefetch=1,
            grid=(nb, 2),
            in_specs=[
                pl.BlockSpec((BQ, 256), lambda i, g, meta: (q_block(base, nb, i, meta), g)),
                pl.BlockSpec((1, keys, 64), lambda i, g, meta: (g, 0, 0)),
                pl.BlockSpec((1, VROWS, keys), lambda i, g, meta: (g, 0, 0)),
            ],
            out_specs=[
                pl.BlockSpec((BQ, 256), lambda i, g, meta: (jnp.minimum(i, hb - 1), jnp.where(i < hb, g, 1))),
                pl.BlockSpec((BQ, 256), lambda i, g, meta: (jnp.maximum(i - hb, 0), jnp.where(i < hb, 0, g))),
            ],
            scratch_shapes=[pltpu.VMEM((4, BK, BQ), F32), pltpu.VMEM((4, VROWS, BQ), F32)],
        ),
        out_shape=[jax.ShapeDtypeStruct((half, 512), BF16)] * 2,
        cost_estimate=pl.CostEstimate(flops=pairs * 700, bytes_accessed=t_chunk * 4096, transcendentals=pairs),
        name="attn",
    )(meta, q, k, vt)


def oproj_kernel(meta_ref, o0_ref, o1_ref, o2_ref, o3_ref, xa_ref, xb_ref, gain_ref, *rest):
    w_parts, (h_ref, m_ref, o_all, w_all, sems) = rest[:8], rest[8:]
    half = xa_ref.shape[1]

    def copies():
        for j in range(4):
            rows = pl.ds(pl.multiple_of(meta_ref[2 + j] * 512, 512), 512)
            for c in range(2):
                yield pltpu.make_async_copy(w_parts[2 * j + c], w_all.at[c, rows, :], sems.at[c, j])

    @pl.when(pl.program_id(0) == 0)
    def _():
        for copy in copies():
            copy.start()

    for j, ref in enumerate((o0_ref, o1_ref, o2_ref, o3_ref)):
        o_all[:, pl.ds(pl.multiple_of(meta_ref[2 + j] * 512, 512), 512)] = ref[...]

    @pl.when(pl.program_id(0) == 0)
    def _():
        for copy in copies():
            copy.wait()

    o = o_all[...]
    ha = (xa_ref[...].astype(F32) + dot(o, w_all[0])).astype(BF16)
    hb = (xb_ref[...].astype(F32) + dot(o, w_all[1])).astype(BF16)
    h_ref[...] = ha
    ha = ha.astype(F32)
    hb = hb.astype(F32)
    row_sq = jnp.sum(ha * ha, axis=-1, keepdims=True) + jnp.sum(hb * hb, axis=-1, keepdims=True)
    scale = lax.rsqrt(row_sq / (2 * half) + NORM_EPS)
    m_ref[:, :half] = (ha * scale * gain_ref[0:1, :].astype(F32)).astype(BF16)
    m_ref[:, half:] = (hb * scale * gain_ref[1:2, :].astype(F32)).astype(BF16)


def oproj_call(chunk, t_chunk, meta, o_parts, xa, xb, w_parts, gains):
    half = xa.shape[1]
    t_half = t_chunk // 2
    bt = min(256, t_half)
    nb = t_half // bt
    o_spec = pl.BlockSpec((bt, 512), lambda i, meta: (i, 0))
    x_spec = pl.BlockSpec((bt, half), lambda i, meta: (chunk * 2 * nb + meta[0] * nb + i, 0))
    return pl.pallas_call(
        oproj_kernel,
        grid_spec=pltpu.PrefetchScalarGridSpec(
            num_scalar_prefetch=1,
            grid=(nb,),
            in_specs=[o_spec] * 4 + [x_spec] * 2 + [whole((2, half))] + [HBM] * 8,
            out_specs=[
                pl.BlockSpec((bt, half), lambda i, meta: (i, 0)),
                pl.BlockSpec((bt, 2 * half), lambda i, meta: (i, 0)),
            ],
            scratch_shapes=[
                pltpu.VMEM((bt, 2048), BF16),
                pltpu.VMEM((2, 2048, half), BF16),
                pltpu.SemaphoreType.DMA((2, 4)),
            ],
        ),
        out_shape=[jax.ShapeDtypeStruct((t_half, half), BF16), jax.ShapeDtypeStruct((t_half, 2 * half), BF16)],
        cost_estimate=pl.CostEstimate(flops=2 * t_half * 2048 * 2048, bytes_accessed=t_half * 8192, transcendentals=0),
        name="oproj",
    )(meta, *o_parts, xa, xb, gains, *w_parts)


def gateup_kernel(nb, mo_ref, mm_ref, ga_ref, gb_ref, ua_ref, ub_ref, act_ref, w_all, sems):
    i = pl.program_id(0)
    half = ga_ref.shape[0]
    srcs = (ga_ref, gb_ref, ua_ref, ub_ref)

    @pl.when(i == 0)
    def _():
        for j in range(4):
            pltpu.make_async_copy(srcs[j], w_all.at[j], sems.at[j]).start()

    def ready(j):
        @pl.when(i == 0)
        def _():
            pltpu.make_async_copy(srcs[j], w_all.at[j], sems.at[j]).wait()

    m = jnp.where(i < nb, mo_ref[...], mm_ref[...])
    ready(0)
    gate = dot(m[:, :half], w_all[0])
    ready(1)
    gate = gate + dot(m[:, half:], w_all[1])
    ready(2)
    up = dot(m[:, :half], w_all[2])
    ready(3)
    up = up + dot(m[:, half:], w_all[3])
    act_ref[...] = (jax.nn.silu(gate) * up).astype(BF16)


def gateup_call(m_own, m_mate, ga, gb, ua, ub):
    t_half, width = m_own.shape
    half = width // 2
    hid = ga.shape[1]
    bt = min(256, t_half)
    nb = t_half // bt
    return pl.pallas_call(
        functools.partial(gateup_kernel, nb),
        grid=(2 * nb,),
        in_specs=[
            pl.BlockSpec((bt, width), lambda i: (jnp.minimum(i, nb - 1), 0)),
            pl.BlockSpec((bt, width), lambda i: (jnp.maximum(i - nb, 0), 0)),
        ]
        + [HBM] * 4,
        out_specs=pl.BlockSpec((bt, hid), lambda i: (i, 0)),
        out_shape=jax.ShapeDtypeStruct((2 * t_half, hid), BF16),
        scratch_shapes=[pltpu.VMEM((4, half, hid), BF16), pltpu.SemaphoreType.DMA((4,))],
        cost_estimate=pl.CostEstimate(flops=2 * 2 * t_half * width * hid * 2, bytes_accessed=t_half * 16384, transcendentals=2 * t_half * hid),
        name="gateup",
    )(m_own, m_mate, ga, gb, ua, ub)


def down_kernel(act_ref, da_ref, db_ref, own_ref, mate_ref, w_all, sems):
    i = pl.program_id(0)
    half = da_ref.shape[1]
    srcs = (da_ref, db_ref)

    @pl.when(i == 0)
    def _():
        for j in range(2):
            pltpu.make_async_copy(srcs[j], w_all.at[j], sems.at[j]).start()

    def ready(j):
        @pl.when(i == 0)
        def _():
            pltpu.make_async_copy(srcs[j], w_all.at[j], sems.at[j]).wait()

    act = act_ref[...]
    ready(0)
    pa = dot(act, w_all[0]).astype(BF16)
    ready(1)
    pb = dot(act, w_all[1]).astype(BF16)

    @pl.when(i == 0)
    def _():
        mate_ref[:, :half] = pa
        mate_ref[:, half:] = pb

    @pl.when(i == 1)
    def _():
        own_ref[:, :half] = pa
        own_ref[:, half:] = pb


def down_call(act, sub, bt, da, db):
    hid, half = da.shape
    per_half = act.shape[0] // 2 // bt
    return pl.pallas_call(
        down_kernel,
        grid=(2,),
        in_specs=[pl.BlockSpec((bt, hid), lambda i: ((1 - i) * per_half + sub, 0)), HBM, HBM],
        out_specs=[pl.BlockSpec((bt, 2 * half), lambda i: (0, 0))] * 2,
        out_shape=[jax.ShapeDtypeStruct((bt, 2 * half), BF16)] * 2,
        scratch_shapes=[pltpu.VMEM((2, hid, half), BF16), pltpu.SemaphoreType.DMA((2,))],
        cost_estimate=pl.CostEstimate(flops=2 * 2 * bt * hid * 2 * half, bytes_accessed=bt * 16384, transcendentals=0),
        name="down",
    )(act, da, db)


def solution(mesh):
    mx_size = mesh.shape["mx"]
    swap_y = [(0, 1), (1, 0)]
    swap_x = [(d, d ^ 2) for d in range(mx_size)]
    swap_c = [(d, d ^ 1) for d in range(mx_size)]
    swap_xc = [(d, d ^ 3) for d in range(mx_size)]

    def local_layer(x_in, gain_attn, w_q, w_k, w_v, w_o, gain_mlp, w_gate, w_up, w_down):
        tokens, half = x_in.shape
        row = lax.axis_index("my")
        me = lax.axis_index("mx")
        core = lax.rem(me, 2)
        meta = jnp.stack([core, me, me, me ^ 1, me ^ 2, me ^ 3]).astype(jnp.int32)
        t_chunk = tokens // CHUNKS
        t_half = t_chunk // 2
        piece = t_chunk // mx_size

        gains = jnp.stack([gain_attn, gain_mlp])
        gains_oth = lax.ppermute(gains, "my", swap_y)
        gains_a = jnp.stack([gain_attn, gains_oth[0]])
        gains_m = jnp.stack([gain_mlp, gains_oth[1]])
        w_qkv = jnp.concatenate([w_q.reshape(half, 512), w_k.reshape(half, 128), w_v.reshape(half, 128)], axis=1)
        w_qkv_oth = lax.ppermute(w_qkv, "my", swap_y)

        x_pieces = []
        for s in range(CHUNKS):
            mine = lax.dynamic_slice(x_in, (s * t_chunk + me * piece, 0), (piece, half))
            got_y = lax.ppermute(mine, "my", swap_y)
            got_x = lax.ppermute(got_y, "mx", swap_x)
            got_c = lax.ppermute(got_y, "mx", swap_c)
            got_xc = lax.ppermute(got_x, "mx", swap_c)
            x_pieces.append((got_y, got_c, got_x, got_xc))

        wo_own = w_o.reshape(512, half)
        wo_x = lax.ppermute(wo_own, "mx", swap_x)
        wo_oth = lax.ppermute(wo_own, "my", swap_y)
        wo_xoth = lax.ppermute(wo_oth, "mx", swap_x)
        wo_parts = [wo_own, wo_oth]
        wo_parts += [lax.ppermute(wo_own, "mx", swap_c), lax.ppermute(wo_oth, "mx", swap_c)]
        wo_parts += [wo_x, wo_xoth]
        wo_parts += [lax.ppermute(wo_x, "mx", swap_c), lax.ppermute(wo_xoth, "mx", swap_c)]

        hid = w_gate.shape[1] // 2
        keep, give = row * hid, (1 - row) * hid
        gb = lax.ppermute(lax.dynamic_slice(w_gate, (0, give), (half, hid)), "my", swap_y)
        ub = lax.ppermute(lax.dynamic_slice(w_up, (0, give), (half, hid)), "my", swap_y)
        db = lax.ppermute(lax.dynamic_slice(w_down, (give, 0), (hid, half)), "my", swap_y)
        ga = lax.dynamic_slice(w_gate, (0, keep), (half, hid))
        ua = lax.dynamic_slice(w_up, (0, keep), (half, hid))
        da = lax.dynamic_slice(w_down, (keep, 0), (hid, half))

        half_dim = 32
        inv_freq = ROPE_BASE ** (-jnp.arange(half_dim, dtype=F32) / half_dim)
        angles = jnp.arange(tokens, dtype=F32)[:, None] * inv_freq[None, :]
        cos_t = jnp.cos(angles)
        sin_t = jnp.sin(angles)
        cos_t = jnp.concatenate([cos_t] * 4, axis=1)
        sin_t = jnp.concatenate([-sin_t, sin_t] * 2, axis=1)

        prev = None
        acts, h_all = [], []
        for ch in range(CHUNKS):
            prev = qkv_call(ch, meta, x_in, x_pieces[ch], w_qkv, w_qkv_oth, gains_a, cos_t, sin_t, prev)
            q, k, vt, x_oth = prev
            o_own, o_mate = attn_call(ch, t_chunk, meta, q, k, vt)
            o_c = lax.ppermute(o_mate, "mx", swap_c)
            o_x = lax.ppermute(o_own, "mx", swap_x)
            o_xc = lax.ppermute(o_mate, "mx", swap_xc)
            h_all.append((o_own, o_c, o_x, o_xc))
        q, k, vt, x_oth = prev
        for ch in range(CHUNKS):
            h_own, m_own = oproj_call(ch, t_chunk, meta, h_all[ch], x_in, x_oth, wo_parts, gains_m)
            h_all[ch] = h_own
            m_mate = lax.ppermute(m_own, "mx", swap_c)
            acts.append(gateup_call(m_own, m_mate, ga, gb, ua, ub))

        sub_rows = t_half // OUT_SUBS
        y_out = x_oth
        for ch in range(CHUNKS):
            for u in range(OUT_SUBS):
                p_own, p_mate = down_call(acts[ch], u, sub_rows, da, db)
                p_recv = lax.ppermute(p_mate, "mx", swap_c)
                s_a = (p_own[:, :half].astype(F32) + p_recv[:, :half].astype(F32)).astype(BF16)
                s_b = (p_own[:, half:].astype(F32) + p_recv[:, half:].astype(F32)).astype(BF16)
                r_y = lax.ppermute(s_b, "my", swap_y)
                z_own = (s_a.astype(F32) + r_y.astype(F32)).astype(BF16)
                z_x = lax.ppermute(z_own, "mx", swap_x)
                h_sub = h_all[ch][u * sub_rows : (u + 1) * sub_rows]
                y_own = (h_sub.astype(F32) + (z_own.astype(F32) + z_x.astype(F32))).astype(BF16)
                y_mate = lax.ppermute(y_own, "mx", swap_c)
                start = ch * t_chunk + u * sub_rows
                y_out = lax.dynamic_update_slice(y_out, y_own, (start + core * t_half, 0))
                y_out = lax.dynamic_update_slice(y_out, y_mate, (start + (1 - core) * t_half, 0))
        return y_out

    in_specs = (P("dp", "my"), P("my"), P("my", "mx", None), P("my", "mx", None), P("my", "mx", None), P("mx", None, "my"), P("my"), P("my", "mx"), P("my", "mx"), P("mx", "my"))
    return jax.shard_map(local_layer, mesh=mesh, in_specs=in_specs, out_specs=P("dp", "my"), check_vma=False)
```
